1024 devices in a mesh: lat: 64 (over y_lo, x, core), lev: 16 (over y_hi, z).
Axes of the slice: x: 8, y: 8 (y_hi: 2, y_lo: 4; y = y_hi * 4 + y_lo), z: 8, core: 2. Of those that a mesh axis runs over, the one named last changes fastest.
Arguments:
- grid: bfloat16 [128, 1024, 2, 2, 8, 128], P(None, 'lat', None, None, None, 'lev'), may hold values from -6 to 6
- legendre: bfloat16 [128, 2, 1024, 512], P('lat'), may hold values from -0.1875 to 0.1875
- quad_weights: float32 [1024], P('lat'), may hold values from 0.25 to 4
- cycle_points: int32 [1024], P('lat'), may hold values from 20 to 4116, as said below
- wave_ids: int32 [128], replicated, may hold values from 0 to 1023, as said below
- mode_projection: bfloat16 [128, 128], replicated, may hold values from -0.5 to 0.5
- vertical_modes: bfloat16 [128, 128], replicated, may hold values from -0.5 to 0.5
- mode_rates: float32 [128], replicated, may hold values from 0.05 to 5
Outputs:
- grid_out: bfloat16 [128, 1024, 2, 2, 8, 128], P(None, 'lat', None, None, None, 'lev')
The draws below stay inside these ranges and needn't reach their ends.
Inputs may be any that keep to these rules, and one draw needn't show every extreme that they name: `cycle_points`: nondecreasing from the first cycle pair to the last; the first cycle pair has the fewest points and the last the most. `wave_ids`: slots 2 i and 2 i + 1 carry wavenumbers m and 1023 - m; no wavenumber appears twice.
All inputs are finite; a program needn't handle non-finite values.
Results may differ from the reference program's by a relative error of at most 0.0073.
Values may be sent and summed in bfloat16 or wider, within the bound.
A program may use at most 64 MiB of HBM per device.

```python
import math
import jax
import jax.numpy as jnp
from jax import lax

HALF = 1024
MODES = 1024
LEVELS = 128
FIELDS = 8
KHALF = 512
SLOTS = 128


def draw_cycle_points(key, part):
    drawn = jax.random.randint(key, (HALF,), 20, 4 * HALF + 21)
    ordered = jnp.sort(drawn)
    ordered = ordered.at[0].set(20)
    ordered = ordered.at[HALF - 1].set(4 * HALF + 20)
    return ordered.astype(jnp.int32)


def draw_wave_ids(key, part):
    pick_key = jax.random.fold_in(key, 11)
    order_key = jax.random.fold_in(key, 23)
    others = 1 + jax.random.permutation(pick_key, MODES // 2 - 1)[:SLOTS // 2 - 1]
    lower_half = jnp.concatenate([jnp.zeros((1,), jnp.int32), others.astype(jnp.int32)])
    lower_half = lower_half[jax.random.permutation(order_key, SLOTS // 2)]
    paired = jnp.stack([lower_half, MODES - 1 - lower_half], axis=1)
    return paired.reshape(SLOTS).astype(jnp.int32)


def steps_of(key, dims, cuts, low, largest):
    gain = 1.0
    for position, shards_of in cuts:
        heights = jax.random.uniform(jax.random.fold_in(jax.random.fold_in(key, 6), position), (shards_of,), jnp.float32, low / len(cuts), largest / len(cuts))
        gain = gain * jnp.repeat(jnp.exp(heights), dims[position] // shards_of).reshape((-1,) + (1,) * (len(dims) - 1 - position))
    return gain


def noise(stream_key, dims, width, most, shards=(), kind=jnp.bfloat16):
    level = steps_of(stream_key, dims, shards, -0.22, 0.18) if shards else 1.0
    values = jax.random.normal(stream_key, dims, jnp.float32) * width * level
    return jnp.minimum(jnp.maximum(values, -most), most).astype(kind)


def setup_inputs(seed: int = 0) -> dict:
    key_of = jax.random.split(jax.random.key(seed), 9)
    grid = noise(key_of[0], (SLOTS, HALF, 2, 2, FIELDS, LEVELS), 1.0, 6.0, ((1, 64), (5, 16)))
    legendre = noise(key_of[1], (SLOTS, 2, HALF, KHALF), HALF ** -0.5, 0.1875, ((0, 64),))
    quad_weights = jnp.clip(jnp.exp(math.log(4.0) - 2.7725887 * jax.random.uniform(key_of[2], (HALF,), jnp.float32) ** steps_of(key_of[2], (HALF,), ((0, 64),), -0.2, 0.2)), 0.25, 4.0)
    cycle_points = draw_cycle_points(jax.random.fold_in(key_of[8], 71), 0)
    wave_ids = draw_wave_ids(jax.random.fold_in(key_of[8], 71), 0)
    mode_projection = noise(key_of[5], (LEVELS, LEVELS), LEVELS ** -0.5, 0.5)
    vertical_modes = noise(key_of[6], (LEVELS, LEVELS), LEVELS ** -0.5, 0.5)
    mode_rates = jnp.clip(jnp.exp(jax.random.uniform(key_of[7], (LEVELS,), jnp.float32, math.log(0.05), math.log(5.0))), 0.05, 5.0)
    return {"grid": grid, "legendre": legendre, "quad_weights": quad_weights, "cycle_points": cycle_points, "wave_ids": wave_ids, "mode_projection": mode_projection, "vertical_modes": vertical_modes, "mode_rates": mode_rates}


coupling = 2.0


def reference(grid, legendre, quad_weights, cycle_points, wave_ids, mode_projection, vertical_modes, mode_rates):
    def one_slot(operands):
        cycle_slab, leg_table, wave_id = operands
        present = (2 * wave_id < cycle_points).astype(jnp.float32)
        weighting = (quad_weights * present)[:, None, None, None]
        north_cycle = cycle_slab[:, 0].astype(jnp.float32)
        south_cycle = cycle_slab[:, 1].astype(jnp.float32)
        even_part = (weighting * (north_cycle + south_cycle)).astype(jnp.bfloat16)
        odd_part = (weighting * (north_cycle - south_cycle)).astype(jnp.bfloat16)
        folded = jnp.stack([even_part, odd_part]).reshape(2, HALF, 2 * FIELDS * LEVELS)
        k_index = jnp.arange(KHALF, dtype=jnp.int32)
        parity = jnp.arange(2, dtype=jnp.int32)
        total_order = wave_id + parity[:, None] + 2 * k_index[None, :]
        inside = total_order <= MODES - 1
        spectral = jnp.einsum("pjk,pjc->pkc", leg_table.astype(jnp.float32), folded.astype(jnp.float32))
        spectral = jnp.where(inside[:, :, None], spectral, 0.0).astype(jnp.bfloat16)
        spectral = spectral.reshape(2, KHALF, 2, FIELDS, LEVELS)
        projected = jnp.einsum("pkcfl,ql->pkcfq", spectral.astype(jnp.float32), mode_projection.astype(jnp.float32))
        order_float = total_order.astype(jnp.float32)
        growth = coupling * order_float * (order_float + 1.0) / (MODES * MODES)
        damped = (projected / (1.0 + growth[:, :, None, None, None] * mode_rates)).astype(jnp.bfloat16)
        solved = jnp.einsum("pkcfq,lq->pkcfl", damped.astype(jnp.float32), vertical_modes.astype(jnp.float32)).astype(jnp.bfloat16)
        returned = jnp.einsum("pjk,pkc->pjc", leg_table.astype(jnp.float32), solved.reshape(2, KHALF, 2 * FIELDS * LEVELS).astype(jnp.float32)).astype(jnp.bfloat16)
        even_back = returned[0].astype(jnp.float32)
        odd_back = returned[1].astype(jnp.float32)
        north_out = present[:, None] * (even_back + odd_back)
        south_out = present[:, None] * (even_back - odd_back)
        return jnp.stack([north_out, south_out], axis=1).reshape(HALF, 2, 2, FIELDS, LEVELS).astype(jnp.bfloat16)

    return lax.map(one_slot, (grid, legendre, wave_ids))
```

```python
import functools

import jax
import jax.numpy as jnp
from jax import lax
from jax.experimental import pallas as pl
from jax.experimental.pallas import tpu as pltpu
from jax.sharding import PartitionSpec as P

MESH = pl.DeviceIdType.MESH
coupling = 2.0
GROUP = 8
LANE_PAD = 128
F32 = jnp.float32
BF16 = jnp.bfloat16


def matmul(a, b):
    return lax.dot_general(a, b, (((1,), (0,)), ((), ())), preferred_element_type=F32)


def matmul_nt(a, b):
    return lax.dot_general(a, b, (((1,), (1,)), ((), ())), preferred_element_type=F32)


def iotas(shape):
    return lax.broadcasted_iota(jnp.int32, shape, 0), lax.broadcasted_iota(jnp.int32, shape, 1)


def unit(condition):
    return jnp.where(condition, 1.0, 0.0).astype(BF16)


def step_kernel(
    n_lat,
    n_lev,
    grid_ref,
    leg_hbm,
    quad_ref,
    cycle_ref,
    wave_ref,
    wave_row_ref,
    project_ref,
    modes_ref,
    rate_ref,
    out_ref,
    leg,
    turned,
    send,
    recv,
    pack_send_0,
    pack_send_1,
    pack_recv_0,
    pack_recv_1,
    solve_send_0,
    solve_send_1,
    solve_recv_0,
    solve_recv_1,
    back_send,
    back_recv,
    flip_0,
    flip_1,
    leg_sem,
    send_sem,
    recv_sem,
):
    lat, lev = lax.axis_index("lat"), lax.axis_index("lev")
    cycles, _, columns, slots = grid_ref.shape
    k_half = leg.shape[3]
    mode_total = 2 * k_half
    rows = cycles * GROUP
    groups = slots // GROUP
    levels = project_ref.shape[0]
    pack_send = (pack_send_0, pack_send_1)
    pack_recv = (pack_recv_0, pack_recv_1)
    solve_send = (solve_send_0, solve_send_1)
    solve_recv = (solve_recv_0, solve_recv_1)
    flips = (flip_0, flip_1)

    barrier = pltpu.get_barrier_semaphore()

    @pl.loop(1, n_lat)
    def _(r):
        pl.semaphore_signal(
            barrier, inc=1, device_id=(lax.rem(lat + r, n_lat), lev), device_id_type=MESH
        )

    @pl.loop(1, n_lev)
    def _(r):
        pl.semaphore_signal(
            barrier, inc=1, device_id=(lat, lax.rem(lev + r, n_lev)), device_id_type=MESH
        )

    leg_copy = pltpu.make_async_copy(leg_hbm, leg, leg_sem)
    leg_copy.start()

    row, col = iotas((columns, columns))
    eye_columns = unit(row == col)
    row, col = iotas((slots, slots))
    eye_slots = unit(row == col)
    row, col = iotas((rows, rows))
    spread = unit(col == (row % cycles) * GROUP + row // cycles)
    collect = unit(col == (row % GROUP) * cycles + row // GROUP)

    def exchange_lat(stage, p, source, target):
        @pl.loop(1, n_lat)
        def _(r):
            peer = lax.rem(lat + r, n_lat)
            pltpu.make_async_remote_copy(
                src_ref=source(peer),
                dst_ref=target(lat),
                send_sem=send_sem.at[stage, p],
                recv_sem=recv_sem.at[stage, p],
                device_id=(peer, lev),
                device_id_type=MESH,
            ).start()

    def exchange_lev(stage, p, source, target):
        @pl.loop(1, n_lev)
        def _(r):
            peer = lax.rem(lev + r, n_lev)
            pltpu.make_async_remote_copy(
                src_ref=source.at[peer],
                dst_ref=target.at[lev],
                send_sem=send_sem.at[stage, p],
                recv_sem=recv_sem.at[stage, p],
                device_id=(lat, peer),
                device_id_type=MESH,
            ).start()

    def wait_all(view, semaphore):
        pltpu.make_async_copy(view, view, semaphore).wait()

    def lat_view(p):
        return send.at[p, pl.ds(0, slots - 2)]

    def lev_view(p):
        return pack_send[p].at[pl.ds(0, n_lev - 1)]

    def own_rows(index):
        return pl.ds(pl.multiple_of(index * cycles, cycles), cycles)

    def fold(p):
        @pl.loop(0, cycles)
        def _(j):
            present = jnp.where(2 * wave_row_ref[...] < cycle_ref[j], quad_ref[j], 0.0)
            north = grid_ref[j, 0].astype(F32)
            south = grid_ref[j, 1].astype(F32)
            total = north + south if p == 0 else north - south
            turned[p, j] = matmul_nt(eye_slots, (present * total).astype(BF16))

        @pl.loop(0, groups)
        def _(g):
            block = turned[p, :, pl.ds(pl.multiple_of(g * GROUP, GROUP), GROUP), :]
            block = block.reshape(rows, columns).astype(BF16)
            moved = matmul(spread, block).astype(BF16)
            send[p, pl.ds(g * GROUP, GROUP)] = moved.reshape(GROUP, cycles, columns)

    def send_fold(p):
        exchange_lat(
            0,
            p,
            lambda peer: send.at[p, pl.ds(2 * peer, 2)],
            lambda me: recv.at[p, :, own_rows(me), :],
        )
        for slot in range(2):
            recv[p, slot, own_rows(lat), :] = send[p, 2 * lat + slot]

    def order(p, slot):
        k_index = lax.broadcasted_iota(jnp.int32, (1, k_half), 1)
        return wave_ref[2 * lat + slot] + p + 2 * k_index

    def forward(p):
        wait_all(lat_view(p), recv_sem.at[0, p])
        parts = []
        for slot in range(2):
            across = matmul_nt(eye_columns, recv[p, slot]).astype(BF16)
            spectral = matmul(across, leg[slot, p])
            parts.append(jnp.where(order(p, slot) <= mode_total - 1, spectral, 0.0))
        flipped = matmul(parts[1].astype(BF16), flips[p][...])
        packed = flipped[:, :k_half] + parts[0]
        pack_send[p][:, :, :k_half] = packed.reshape(n_lev, GROUP, k_half).astype(BF16)
        if flipped.shape[1] > k_half:
            rest = flipped[:, k_half:]
            pack_send[p][:, :, k_half:] = rest.reshape(n_lev, GROUP, -1).astype(BF16)
        exchange_lev(1, p, pack_send[p], pack_recv[p])
        pack_recv[p][lev] = pack_send[p][lev]

    def solve(p):
        wait_all(lev_view(p), recv_sem.at[1, p])
        packed = pack_recv[p][...].astype(F32).reshape(levels, -1).astype(BF16)
        width = packed.shape[1]
        q_index = lax.broadcasted_iota(jnp.int32, (1, width), 1)
        first = wave_ref[2 * lat] + p + 2 * q_index
        second = wave_ref[2 * lat + 1] + p + 2 * (k_half - p - q_index)
        total_order = jnp.where(first <= mode_total - 1, first, second).astype(F32)
        growth = coupling * total_order * (total_order + 1.0) / (mode_total * mode_total)
        rates = jnp.transpose(jnp.broadcast_to(rate_ref[...], (levels, levels)))[:, :1]
        projected = matmul(project_ref[...], packed)
        damped = (projected / (1.0 + growth * rates)).astype(BF16)
        solved = matmul(modes_ref[...], damped)
        solve_send[p][...] = solved.reshape(n_lev, GROUP, width).astype(BF16)
        exchange_lev(2, p, solve_send[p], solve_recv[p])
        solve_recv[p][lev] = solve_send[p][lev]

    def inverse(p):
        wait_all(lev_view(p), recv_sem.at[2, p])
        packed = solve_recv[p][...].astype(F32).reshape(columns, -1)
        unpacked = (packed[:, :k_half], matmul_nt(packed.astype(BF16), flips[p][...]))
        for slot in range(2):
            coeffs = jnp.where(order(p, slot) <= mode_total - 1, unpacked[slot], 0.0)
            back_send[p, slot] = matmul_nt(leg[slot, p], coeffs.astype(BF16)).astype(BF16)
        exchange_lat(
            3,
            p,
            lambda peer: back_send.at[p, :, own_rows(peer), :],
            lambda me: back_recv.at[p, pl.ds(2 * me, 2)],
        )
        for slot in range(2):
            back_recv[p, 2 * lat + slot] = back_send[p, slot, own_rows(lat), :]

    def spread_back(p):
        wait_all(lat_view(p), recv_sem.at[3, p])

        @pl.loop(0, groups)
        def _(g):
            block = back_recv[p, pl.ds(g * GROUP, GROUP)].reshape(rows, columns)
            moved = matmul(collect, block).reshape(cycles, GROUP, columns)
            turned[p, :, pl.ds(pl.multiple_of(g * GROUP, GROUP), GROUP), :] = moved

    def unfold():
        @pl.loop(0, cycles)
        def _(j):
            present = jnp.where(2 * wave_row_ref[...] < cycle_ref[j], 1.0, 0.0)
            even = matmul_nt(eye_columns, turned[0, j].astype(BF16))
            odd = matmul_nt(eye_columns, turned[1, j].astype(BF16))
            out_ref[j, 0] = (present * (even + odd)).astype(BF16)
            out_ref[j, 1] = (present * (even - odd)).astype(BF16)

    fold(0)
    pl.semaphore_wait(barrier, n_lat + n_lev - 2)
    send_fold(0)
    fold(1)
    send_fold(1)
    for p in range(2):
        row, col = iotas(flips[p].shape)
        flips[p][...] = unit(row + col == k_half - p)
    leg_copy.wait()
    forward(0)
    solve(0)
    inverse(0)
    forward(1)
    solve(1)
    inverse(1)
    spread_back(0)
    spread_back(1)
    unfold()
    for p in range(2):
        wait_all(lat_view(p), send_sem.at[0, p])
        wait_all(lev_view(p), send_sem.at[1, p])
        wait_all(lev_view(p), send_sem.at[2, p])
        wait_all(lat_view(p), send_sem.at[3, p])


def local(
    n_lat,
    n_lev,
    grid,
    legendre,
    quad_weights,
    cycle_points,
    wave_ids,
    mode_projection,
    vertical_modes,
    mode_rates,
):
    slots, cycles, _, parts, fields, levels_local = grid.shape
    columns = parts * fields * levels_local
    k_half = legendre.shape[3]
    widths = (k_half + LANE_PAD, k_half)
    held = jnp.transpose(grid, (1, 2, 3, 4, 5, 0)).reshape(cycles, 2, columns, slots)
    vmem = pl.BlockSpec(memory_space=pltpu.VMEM)
    smem = pl.BlockSpec(memory_space=pltpu.SMEM)
    packs = [pltpu.VMEM((n_lev, GROUP, width), BF16) for width in widths]
    out = pl.pallas_call(
        functools.partial(step_kernel, n_lat, n_lev),
        out_shape=jax.ShapeDtypeStruct((cycles, 2, columns, slots), BF16),
        in_specs=[vmem, pl.BlockSpec(memory_space=pl.ANY), smem, smem, smem, vmem, vmem, vmem, vmem],
        out_specs=vmem,
        scratch_shapes=[
            pltpu.VMEM(legendre.shape, BF16),
            pltpu.VMEM((2, cycles, slots, columns), F32),
            pltpu.VMEM((2, slots, cycles, columns), BF16),
            pltpu.VMEM((2, 2, n_lat * cycles, columns), BF16),
            *packs,
            *packs,
            *packs,
            *packs,
            pltpu.VMEM((2, 2, n_lat * cycles, columns), BF16),
            pltpu.VMEM((2, slots, cycles, columns), BF16),
            *[pltpu.VMEM((k_half, width), BF16) for width in widths],
            pltpu.SemaphoreType.DMA,
            pltpu.SemaphoreType.DMA((4, 2)),
            pltpu.SemaphoreType.DMA((4, 2)),
        ],
        compiler_params=pltpu.CompilerParams(
            collective_id=0, has_side_effects=True, vmem_limit_bytes=48 * 1024 * 1024
        ),
        name="spectral_step",
    )(
        held,
        legendre,
        quad_weights,
        cycle_points,
        wave_ids,
        wave_ids.reshape(1, slots),
        mode_projection,
        vertical_modes,
        mode_rates.reshape(1, -1),
    )
    out = out.reshape(cycles, 2, parts, fields, levels_local, slots)
    return jnp.transpose(out, (5, 0, 1, 2, 3, 4))


def solution(mesh):
    placed = (
        P(None, "lat", None, None, None, "lev"),
        P("lat", None, None, None),
        P("lat"),
        P("lat"),
        P(),
        P(),
        P(),
        P(),
    )
    return jax.shard_map(
        functools.partial(local, mesh.shape["lat"], mesh.shape["lev"]),
        mesh=mesh,
        in_specs=placed,
        out_specs=P(None, "lat", None, None, None, "lev"),
        check_vma=False,
    )
```

```python
import functools

import jax
import jax.numpy as jnp
from jax import lax
from jax.experimental import pallas as pl
from jax.experimental.pallas import tpu as pltpu
from jax.sharding import PartitionSpec as P

MESH = pl.DeviceIdType.MESH
coupling = 2.0
GROUP = 8
LANE_PAD = 128
F32 = jnp.float32
BF16 = jnp.bfloat16


def matmul(a, b):
    return lax.dot_general(a, b, (((1,), (0,)), ((), ())), preferred_element_type=F32)


def matmul_nt(a, b):
    return lax.dot_general(a, b, (((1,), (1,)), ((), ())), preferred_element_type=F32)


def iotas(shape):
    return lax.broadcasted_iota(jnp.int32, shape, 0), lax.broadcasted_iota(jnp.int32, shape, 1)


def unit(condition):
    return jnp.where(condition, 1.0, 0.0).astype(BF16)


def step_kernel(
    n_lat,
    n_lev,
    grid_hbm,
    leg_hbm,
    quad_hbm,
    cycle_hbm,
    wave_hbm,
    wave_row_hbm,
    project_hbm,
    modes_hbm,
    rate_hbm,
    out_hbm,
    grid_ref,
    leg,
    quad_ref,
    cycle_ref,
    wave_ref,
    wave_row_ref,
    project_ref,
    modes_ref,
    rate_ref,
    turned,
    even_ref,
    send,
    recv,
    pack_send_0,
    pack_send_1,
    pack_recv_0,
    pack_recv_1,
    solve_send_0,
    solve_send_1,
    solve_recv_0,
    solve_recv_1,
    back_send,
    back_recv,
    flip_0,
    flip_1,
    grid_sem,
    input_sem,
    send_sem,
    recv_sem,
):
    lat, lev = lax.axis_index("lat"), lax.axis_index("lev")
    cycles, _, columns, slots = grid_hbm.shape
    k_half = leg.shape[3]
    mode_total = 2 * k_half
    rows = cycles * GROUP
    groups = slots // GROUP
    levels = project_ref.shape[0]
    pack_send = (pack_send_0, pack_send_1)
    pack_recv = (pack_recv_0, pack_recv_1)
    solve_send = (solve_send_0, solve_send_1)
    solve_recv = (solve_recv_0, solve_recv_1)
    flips = (flip_0, flip_1)

    def grid_copy(j):
        return pltpu.make_async_copy(grid_hbm.at[j], grid_ref.at[j], grid_sem.at[j])

    inputs = [
        (wave_row_hbm, wave_row_ref),
        (cycle_hbm, cycle_ref),
        (quad_hbm, quad_ref),
        (wave_hbm, wave_ref),
        (leg_hbm, leg),
        (project_hbm, project_ref),
        (modes_hbm, modes_ref),
        (rate_hbm, rate_ref),
    ]
    copies = [
        pltpu.make_async_copy(source, target, input_sem.at[i])
        for i, (source, target) in enumerate(inputs)
    ]
    for copy in copies[:3]:
        copy.start()

    @pl.loop(0, cycles)
    def _(j):
        grid_copy(j).start()

    for copy in copies[3:]:
        copy.start()

    barrier = pltpu.get_barrier_semaphore()

    @pl.loop(1, n_lat)
    def _(r):
        pl.semaphore_signal(
            barrier, inc=1, device_id=(lax.rem(lat + r, n_lat), lev), device_id_type=MESH
        )

    @pl.loop(1, n_lev)
    def _(r):
        pl.semaphore_signal(
            barrier, inc=1, device_id=(lat, lax.rem(lev + r, n_lev)), device_id_type=MESH
        )


    row, col = iotas((columns, columns))
    eye_columns = unit(row == col)
    row, col = iotas((slots, slots))
    eye_slots = unit(row == col)
    row, col = iotas((rows, rows))
    spread = unit(col == (row % cycles) * GROUP + row // cycles)
    collect = unit(col == (row % GROUP) * cycles + row // GROUP)

    x_size = min(8, n_lat // 2)
    y_size = n_lat // (2 * x_size)
    at_core, at_x, at_y = lax.rem(lat, 2), lax.rem(lat // 2, x_size), lat // (2 * x_size)
    shifts = sorted(range(x_size), key=lambda d: -min(d, x_size - d))

    def exchange_lat(stage, p, source, target):
        for shift in shifts:
            to_x = lax.rem(at_x + shift, x_size)

            @pl.loop(0 if shift else 1, 2 * y_size)
            def _(t):
                to_y = lax.rem(at_y + t // 2, y_size)
                peer = (to_y * x_size + to_x) * 2 + lax.rem(at_core + t, 2)
                pltpu.make_async_remote_copy(
                    src_ref=source(peer),
                    dst_ref=target(lat),
                    send_sem=send_sem.at[stage, p],
                    recv_sem=recv_sem.at[stage, p],
                    device_id=(peer, lev),
                    device_id_type=MESH,
                ).start()

    def exchange_lev(stage, p, source, target):
        @pl.loop(1, n_lev)
        def _(r):
            peer = lax.rem(lev + r, n_lev)
            pltpu.make_async_remote_copy(
                src_ref=source.at[peer],
                dst_ref=target.at[lev],
                send_sem=send_sem.at[stage, p],
                recv_sem=recv_sem.at[stage, p],
                device_id=(lat, peer),
                device_id_type=MESH,
            ).start()

    def wait_all(view, semaphore):
        pltpu.make_async_copy(view, view, semaphore).wait()

    def lat_view(p):
        return send.at[p, pl.ds(0, slots - 2)]

    def lev_view(p):
        return pack_send[p].at[pl.ds(0, n_lev - 1)]

    def own_rows(index):
        return pl.ds(pl.multiple_of(index * cycles, cycles), cycles)

    def fold(p):
        @pl.loop(0, cycles, unroll=4)
        def _(j):
            if p == 0:
                grid_copy(j).wait()
            present = jnp.where(2 * wave_row_ref[...] < cycle_ref[j], quad_ref[j], 0.0)
            north = grid_ref[j, 0].astype(F32)
            south = grid_ref[j, 1].astype(F32)
            total = north + south if p == 0 else north - south
            turned[p, j] = matmul_nt(eye_slots, (present * total).astype(BF16))

        @pl.loop(0, groups, unroll=4)
        def _(g):
            block = turned[p, :, pl.ds(pl.multiple_of(g * GROUP, GROUP), GROUP), :]
            block = block.reshape(rows, columns).astype(BF16)
            moved = matmul(spread, block).astype(BF16)
            send[p, pl.ds(g * GROUP, GROUP)] = moved.reshape(GROUP, cycles, columns)

    def send_fold(p):
        exchange_lat(
            0,
            p,
            lambda peer: send.at[p, pl.ds(2 * peer, 2)],
            lambda me: recv.at[p, :, own_rows(me), :],
        )
        for slot in range(2):
            recv[p, slot, own_rows(lat), :] = send[p, 2 * lat + slot]

    def order(p, slot):
        k_index = lax.broadcasted_iota(jnp.int32, (1, k_half), 1)
        return wave_ref[2 * lat + slot] + p + 2 * k_index

    def forward(p):
        wait_all(lat_view(p), recv_sem.at[0, p])
        parts = []
        for slot in range(2):
            across = matmul_nt(eye_columns, recv[p, slot]).astype(BF16)
            spectral = matmul(across, leg[slot, p])
            parts.append(jnp.where(order(p, slot) <= mode_total - 1, spectral, 0.0))
        flipped = matmul(parts[1].astype(BF16), flips[p][...])
        packed = flipped[:, :k_half] + parts[0]
        pack_send[p][:, :, :k_half] = packed.reshape(n_lev, GROUP, k_half).astype(BF16)
        if flipped.shape[1] > k_half:
            rest = flipped[:, k_half:]
            pack_send[p][:, :, k_half:] = rest.reshape(n_lev, GROUP, -1).astype(BF16)
        exchange_lev(1, p, pack_send[p], pack_recv[p])
        pack_recv[p][lev] = pack_send[p][lev]

    def solve(p):
        wait_all(lev_view(p), recv_sem.at[1, p])
        packed = pack_recv[p][...].astype(F32).reshape(levels, -1).astype(BF16)
        width = packed.shape[1]
        q_index = lax.broadcasted_iota(jnp.int32, (1, width), 1)
        first = wave_ref[2 * lat] + p + 2 * q_index
        second = wave_ref[2 * lat + 1] + p + 2 * (k_half - p - q_index)
        total_order = jnp.where(first <= mode_total - 1, first, second).astype(F32)
        growth = coupling * total_order * (total_order + 1.0) / (mode_total * mode_total)
        rates = jnp.transpose(jnp.broadcast_to(rate_ref[...], (levels, levels)))[:, :1]
        projected = matmul(project_ref[...], packed)
        damped = (projected / (1.0 + growth * rates)).astype(BF16)
        solved = matmul(modes_ref[...], damped)
        solve_send[p][...] = solved.reshape(n_lev, GROUP, width).astype(BF16)
        exchange_lev(2, p, solve_send[p], solve_recv[p])
        solve_recv[p][lev] = solve_send[p][lev]

    def inverse(p):
        wait_all(lev_view(p), recv_sem.at[2, p])
        packed = solve_recv[p][...].astype(F32).reshape(columns, -1)
        unpacked = (packed[:, :k_half], matmul_nt(packed.astype(BF16), flips[p][...]))
        for slot in range(2):
            coeffs = jnp.where(order(p, slot) <= mode_total - 1, unpacked[slot], 0.0)
            back_send[p, slot] = matmul_nt(leg[slot, p], coeffs.astype(BF16)).astype(BF16)
        exchange_lat(
            3,
            p,
            lambda peer: back_send.at[p, :, own_rows(peer), :],
            lambda me: back_recv.at[p, pl.ds(2 * me, 2)],
        )
        for slot in range(2):
            back_recv[p, 2 * lat + slot] = back_send[p, slot, own_rows(lat), :]

    def spread_back(p):
        wait_all(lat_view(p), recv_sem.at[3, p])

        @pl.loop(0, groups, unroll=4)
        def _(g):
            block = back_recv[p, pl.ds(g * GROUP, GROUP)].reshape(rows, columns)
            moved = matmul(collect, block).reshape(cycles, GROUP, columns)
            turned[p, :, pl.ds(pl.multiple_of(g * GROUP, GROUP), GROUP), :] = moved

    def cross(p, j):
        return matmul_nt(eye_columns, turned[p, j].astype(BF16))

    def out_copy(j):
        return pltpu.make_async_copy(grid_ref.at[j], out_hbm.at[j], grid_sem.at[j])

    def turn_even():
        @pl.loop(0, cycles, unroll=4)
        def _(j):
            even_ref[j] = cross(0, j)

    def unfold():
        @pl.loop(0, cycles, unroll=4)
        def _(j):
            present = jnp.where(2 * wave_row_ref[...] < cycle_ref[j], 1.0, 0.0)
            even, odd = even_ref[j], cross(1, j)
            grid_ref[j, 0] = (present * (even + odd)).astype(BF16)
            grid_ref[j, 1] = (present * (even - odd)).astype(BF16)
            out_copy(j).start()

    for copy in copies[:3]:
        copy.wait()
    fold(0)
    pl.semaphore_wait(barrier, n_lat + n_lev - 2)
    send_fold(0)
    fold(1)
    send_fold(1)
    for p in range(2):
        row, col = iotas(flips[p].shape)
        flips[p][...] = unit(row + col == k_half - p)
    for copy in copies[3:]:
        copy.wait()
    forward(0)
    solve(0)
    forward(1)
    inverse(0)
    solve(1)
    inverse(1)
    spread_back(0)
    turn_even()
    spread_back(1)
    unfold()
    for p in range(2):
        wait_all(lat_view(p), send_sem.at[0, p])
        wait_all(lev_view(p), send_sem.at[1, p])
        wait_all(lev_view(p), send_sem.at[2, p])
        wait_all(lat_view(p), send_sem.at[3, p])

    @pl.loop(0, cycles)
    def _(j):
        out_copy(j).wait()


def local(
    n_lat,
    n_lev,
    grid,
    legendre,
    quad_weights,
    cycle_points,
    wave_ids,
    mode_projection,
    vertical_modes,
    mode_rates,
):
    slots, cycles, _, parts, fields, levels_local = grid.shape
    columns = parts * fields * levels_local
    k_half = legendre.shape[3]
    widths = (k_half + LANE_PAD, k_half)
    held = jnp.transpose(grid, (1, 2, 3, 4, 5, 0)).reshape(cycles, 2, columns, slots)
    hbm = pl.BlockSpec(memory_space=pltpu.HBM)
    packs = [pltpu.VMEM((n_lev, GROUP, width), BF16) for width in widths]
    out = pl.pallas_call(
        functools.partial(step_kernel, n_lat, n_lev),
        out_shape=jax.ShapeDtypeStruct((cycles, 2, columns, slots), BF16),
        in_specs=[hbm] * 9,
        out_specs=hbm,
        scratch_shapes=[
            pltpu.VMEM(held.shape, BF16),
            pltpu.VMEM(legendre.shape, BF16),
            pltpu.SMEM(quad_weights.shape, F32),
            pltpu.SMEM(cycle_points.shape, jnp.int32),
            pltpu.SMEM(wave_ids.shape, jnp.int32),
            pltpu.VMEM((1, slots), jnp.int32),
            pltpu.VMEM(mode_projection.shape, BF16),
            pltpu.VMEM(vertical_modes.shape, BF16),
            pltpu.VMEM((1, mode_rates.shape[0]), F32),
            pltpu.VMEM((2, cycles, slots, columns), F32),
            pltpu.VMEM((cycles, columns, slots), F32),
            pltpu.VMEM((2, slots, cycles, columns), BF16),
            pltpu.VMEM((2, 2, n_lat * cycles, columns), BF16),
            *packs,
            *packs,
            *packs,
            *packs,
            pltpu.VMEM((2, 2, n_lat * cycles, columns), BF16),
            pltpu.VMEM((2, slots, cycles, columns), BF16),
            *[pltpu.VMEM((k_half, width), BF16) for width in widths],
            pltpu.SemaphoreType.DMA((cycles,)),
            pltpu.SemaphoreType.DMA((8,)),
            pltpu.SemaphoreType.DMA((4, 2)),
            pltpu.SemaphoreType.DMA((4, 2)),
        ],
        compiler_params=pltpu.CompilerParams(
            collective_id=0, has_side_effects=True, vmem_limit_bytes=62914560
        ),
        name="spectral_step",
    )(
        held,
        legendre,
        quad_weights,
        cycle_points,
        wave_ids,
        wave_ids.reshape(1, slots),
        mode_projection,
        vertical_modes,
        mode_rates.reshape(1, -1),
    )
    out = out.reshape(cycles, 2, parts, fields, levels_local, slots)
    return jnp.transpose(out, (5, 0, 1, 2, 3, 4))


def solution(mesh):
    placed = (
        P(None, "lat", None, None, None, "lev"),
        P("lat", None, None, None),
        P("lat"),
        P("lat"),
        P(),
        P(),
        P(),
        P(),
    )
    return jax.shard_map(
        functools.partial(local, mesh.shape["lat"], mesh.shape["lev"]),
        mesh=mesh,
        in_specs=placed,
        out_specs=P(None, "lat", None, None, None, "lev"),
        check_vma=False,
    )
```

```python
import functools

import jax
import jax.numpy as jnp
from jax import lax
from jax.experimental import pallas as pl
from jax.experimental.pallas import tpu as pltpu
from jax.sharding import PartitionSpec as P

MESH = pl.DeviceIdType.MESH
coupling = 2.0
GROUP = 8
LANE_PAD = 128
F32 = jnp.float32
BF16 = jnp.bfloat16


def matmul(a, b):
    return lax.dot_general(a, b, (((1,), (0,)), ((), ())), preferred_element_type=F32)


def matmul_nt(a, b):
    return lax.dot_general(a, b, (((1,), (1,)), ((), ())), preferred_element_type=F32)


def iotas(shape):
    return lax.broadcasted_iota(jnp.int32, shape, 0), lax.broadcasted_iota(jnp.int32, shape, 1)


def unit(condition):
    return jnp.where(condition, 1.0, 0.0).astype(BF16)


def step_kernel(
    n_lat,
    n_lev,
    grid_hbm,
    leg_hbm,
    quad_hbm,
    cycle_hbm,
    wave_hbm,
    wave_row_hbm,
    project_hbm,
    modes_hbm,
    rate_hbm,
    out_hbm,
    grid_ref,
    leg,
    quad_ref,
    cycle_ref,
    wave_ref,
    wave_row_ref,
    project_ref,
    modes_ref,
    rate_ref,
    turned,
    even_ref,
    send,
    recv,
    pack_send_0,
    pack_send_1,
    pack_recv_0,
    pack_recv_1,
    solve_send_0,
    solve_send_1,
    solve_recv_0,
    solve_recv_1,
    back_send,
    back_recv,
    flip_0,
    flip_1,
    grid_sem,
    input_sem,
    send_sem,
    recv_sem,
):
    lat, lev = lax.axis_index("lat"), lax.axis_index("lev")
    cycles, _, columns, slots = grid_hbm.shape
    k_half = leg.shape[3]
    mode_total = 2 * k_half
    rows = cycles * GROUP
    groups = slots // GROUP
    levels = project_ref.shape[0]
    pack_send = (pack_send_0, pack_send_1)
    pack_recv = (pack_recv_0, pack_recv_1)
    solve_send = (solve_send_0, solve_send_1)
    solve_recv = (solve_recv_0, solve_recv_1)
    flips = (flip_0, flip_1)

    def grid_copy(j):
        return pltpu.make_async_copy(grid_hbm.at[j], grid_ref.at[j], grid_sem.at[j])

    inputs = [
        (wave_row_hbm, wave_row_ref),
        (cycle_hbm, cycle_ref),
        (quad_hbm, quad_ref),
        (wave_hbm, wave_ref),
        (leg_hbm, leg),
        (project_hbm, project_ref),
        (modes_hbm, modes_ref),
        (rate_hbm, rate_ref),
    ]
    copies = [
        pltpu.make_async_copy(source, target, input_sem.at[i])
        for i, (source, target) in enumerate(inputs)
    ]
    for copy in copies[:3]:
        copy.start()

    @pl.loop(0, cycles)
    def _(j):
        grid_copy(j).start()

    for copy in copies[3:]:
        copy.start()

    barrier = pltpu.get_barrier_semaphore()

    @pl.loop(1, n_lat)
    def _(r):
        pl.semaphore_signal(
            barrier, inc=1, device_id=(lax.rem(lat + r, n_lat), lev), device_id_type=MESH
        )

    @pl.loop(1, n_lev)
    def _(r):
        pl.semaphore_signal(
            barrier, inc=1, device_id=(lat, lax.rem(lev + r, n_lev)), device_id_type=MESH
        )


    row, col = iotas((columns, columns))
    eye_columns = unit(row == col)
    row, col = iotas((slots, slots))
    eye_slots = unit(row == col)
    row, col = iotas((rows, rows))
    spread = unit(col == (row % cycles) * GROUP + row // cycles)
    collect = unit(col == (row % GROUP) * cycles + row // GROUP)

    x_size = min(8, n_lat // 2)
    y_size = n_lat // (2 * x_size)
    at_core, at_x, at_y = lax.rem(lat, 2), lax.rem(lat // 2, x_size), lat // (2 * x_size)
    near_last = sorted(range(x_size), key=lambda d: -min(d, x_size - d))
    if x_size == 8:
        split_forward = ((3, 5, 2, 6), (4, 1, 7, 0))
        split_return = ((3, 5), (4, 2, 6, 1, 7, 0))
    else:
        split_forward = split_return = (near_last[:-1], near_last[-1:])

    def exchange_lat(stage, p, shifts, source, target):
        for shift in shifts:
            to_x = lax.rem(at_x + shift, x_size)

            @pl.loop(0 if shift else 1, 2 * y_size)
            def _(t):
                to_y = lax.rem(at_y + t // 2, y_size)
                peer = (to_y * x_size + to_x) * 2 + lax.rem(at_core + t, 2)
                pltpu.make_async_remote_copy(
                    src_ref=source(peer),
                    dst_ref=target(lat),
                    send_sem=send_sem.at[stage, p],
                    recv_sem=recv_sem.at[stage, p],
                    device_id=(peer, lev),
                    device_id_type=MESH,
                ).start()

    z_size = n_lev // 2
    at_z, at_half = lax.rem(lev, z_size), lev // z_size
    hops = sorted(range(z_size), key=lambda d: -min(d, z_size - d))
    lev_steps = [(half, hop) for half in (1, 0) for hop in hops if half or hop]

    def exchange_lev(stage, p, source, target):
        for half, hop in lev_steps:
            peer = lax.rem(at_half + half, 2) * z_size + lax.rem(at_z + hop, z_size)
            pltpu.make_async_remote_copy(
                src_ref=source.at[peer],
                dst_ref=target.at[lev],
                send_sem=send_sem.at[stage, p],
                recv_sem=recv_sem.at[stage, p],
                device_id=(lat, peer),
                device_id_type=MESH,
            ).start()

    def wait_all(view, semaphore):
        pltpu.make_async_copy(view, view, semaphore).wait()

    def lat_view(p):
        return send.at[p, pl.ds(0, slots - 2)]

    def lev_view(p):
        return pack_send[p].at[pl.ds(0, n_lev - 1)]

    def own_rows(index):
        return pl.ds(pl.multiple_of(index * cycles, cycles), cycles)

    def fold(p):
        @pl.loop(0, cycles, unroll=4)
        def _(j):
            if p == 0:
                grid_copy(j).wait()
            present = jnp.where(2 * wave_row_ref[...] < cycle_ref[j], quad_ref[j], 0.0)
            north = grid_ref[j, 0].astype(F32)
            south = grid_ref[j, 1].astype(F32)
            total = north + south if p == 0 else north - south
            turned[p, j] = matmul_nt(eye_slots, (present * total).astype(BF16))

        @pl.loop(0, groups, unroll=4)
        def _(g):
            block = turned[p, :, pl.ds(pl.multiple_of(g * GROUP, GROUP), GROUP), :]
            block = block.reshape(rows, columns).astype(BF16)
            moved = matmul(spread, block).astype(BF16)
            send[p, pl.ds(g * GROUP, GROUP)] = moved.reshape(GROUP, cycles, columns)

    def send_fold(p, shifts):
        exchange_lat(
            0,
            p,
            shifts,
            lambda peer: send.at[p, pl.ds(2 * peer, 2)],
            lambda me: recv.at[p, :, own_rows(me), :],
        )

    def keep_fold(p):
        for slot in range(2):
            recv[p, slot, own_rows(lat), :] = send[p, 2 * lat + slot]

    def order(p, slot):
        k_index = lax.broadcasted_iota(jnp.int32, (1, k_half), 1)
        return wave_ref[2 * lat + slot] + p + 2 * k_index

    def forward(p):
        wait_all(lat_view(p), recv_sem.at[0, p])
        parts = []
        for slot in range(2):
            across = matmul_nt(eye_columns, recv[p, slot]).astype(BF16)
            spectral = matmul(across, leg[slot, p])
            parts.append(jnp.where(order(p, slot) <= mode_total - 1, spectral, 0.0))
        flipped = matmul(parts[1].astype(BF16), flips[p][...])
        packed = flipped[:, :k_half] + parts[0]
        pack_send[p][:, :, :k_half] = packed.reshape(n_lev, GROUP, k_half).astype(BF16)
        if flipped.shape[1] > k_half:
            rest = flipped[:, k_half:]
            pack_send[p][:, :, k_half:] = rest.reshape(n_lev, GROUP, -1).astype(BF16)
        exchange_lev(1, p, pack_send[p], pack_recv[p])
        pack_recv[p][lev] = pack_send[p][lev]

    def solve(p):
        wait_all(lev_view(p), recv_sem.at[1, p])
        packed = pack_recv[p][...].astype(F32).reshape(levels, -1).astype(BF16)
        width = packed.shape[1]
        q_index = lax.broadcasted_iota(jnp.int32, (1, width), 1)
        first = wave_ref[2 * lat] + p + 2 * q_index
        second = wave_ref[2 * lat + 1] + p + 2 * (k_half - p - q_index)
        total_order = jnp.where(first <= mode_total - 1, first, second).astype(F32)
        growth = coupling * total_order * (total_order + 1.0) / (mode_total * mode_total)
        rates = jnp.transpose(jnp.broadcast_to(rate_ref[...], (levels, levels)))[:, :1]
        projected = matmul(project_ref[...], packed)
        damped = (projected / (1.0 + growth * rates)).astype(BF16)
        solved = matmul(modes_ref[...], damped)
        solve_send[p][...] = solved.reshape(n_lev, GROUP, width).astype(BF16)
        exchange_lev(2, p, solve_send[p], solve_recv[p])
        solve_recv[p][lev] = solve_send[p][lev]

    def inverse(p):
        wait_all(lev_view(p), recv_sem.at[2, p])
        packed = solve_recv[p][...].astype(F32).reshape(columns, -1)
        unpacked = (packed[:, :k_half], matmul_nt(packed.astype(BF16), flips[p][...]))
        for slot in range(2):
            coeffs = jnp.where(order(p, slot) <= mode_total - 1, unpacked[slot], 0.0)
            back_send[p, slot] = matmul_nt(leg[slot, p], coeffs.astype(BF16)).astype(BF16)

    def send_back(p, shifts):
        exchange_lat(
            3,
            p,
            shifts,
            lambda peer: back_send.at[p, :, own_rows(peer), :],
            lambda me: back_recv.at[p, pl.ds(2 * me, 2)],
        )

    def keep_back(p):
        for slot in range(2):
            back_recv[p, 2 * lat + slot] = back_send[p, slot, own_rows(lat), :]

    def spread_back(p):
        wait_all(lat_view(p), recv_sem.at[3, p])

        @pl.loop(0, groups, unroll=4)
        def _(g):
            block = back_recv[p, pl.ds(g * GROUP, GROUP)].reshape(rows, columns)
            moved = matmul(collect, block).reshape(cycles, GROUP, columns)
            turned[p, :, pl.ds(pl.multiple_of(g * GROUP, GROUP), GROUP), :] = moved

    def cross(p, j):
        return matmul_nt(eye_columns, turned[p, j].astype(BF16))

    def out_copy(j):
        return pltpu.make_async_copy(grid_ref.at[j], out_hbm.at[j], grid_sem.at[j])

    def turn_even():
        @pl.loop(0, cycles, unroll=4)
        def _(j):
            even_ref[j] = cross(0, j)

    def unfold():
        @pl.loop(0, cycles, unroll=4)
        def _(j):
            present = jnp.where(2 * wave_row_ref[...] < cycle_ref[j], 1.0, 0.0)
            even, odd = even_ref[j], cross(1, j)
            grid_ref[j, 0] = (present * (even + odd)).astype(BF16)
            grid_ref[j, 1] = (present * (even - odd)).astype(BF16)
            out_copy(j).start()

    for copy in copies[:3]:
        copy.wait()
    fold(0)
    pl.semaphore_wait(barrier, n_lat + n_lev - 2)
    send_fold(0, near_last)
    keep_fold(0)
    fold(1)
    send_fold(1, split_forward[0])
    keep_fold(1)
    for p in range(2):
        row, col = iotas(flips[p].shape)
        flips[p][...] = unit(row + col == k_half - p)
    for copy in copies[3:]:
        copy.wait()
    forward(0)
    send_fold(1, split_forward[1])
    solve(0)
    forward(1)
    inverse(0)
    send_back(0, split_return[0])
    keep_back(0)
    solve(1)
    send_back(0, split_return[1])
    inverse(1)
    send_back(1, near_last)
    keep_back(1)
    spread_back(0)
    turn_even()
    spread_back(1)
    unfold()
    for p in range(2):
        wait_all(lat_view(p), send_sem.at[0, p])
        wait_all(lev_view(p), send_sem.at[1, p])
        wait_all(lev_view(p), send_sem.at[2, p])
        wait_all(lat_view(p), send_sem.at[3, p])

    @pl.loop(0, cycles)
    def _(j):
        out_copy(j).wait()


def local(
    n_lat,
    n_lev,
    grid,
    legendre,
    quad_weights,
    cycle_points,
    wave_ids,
    mode_projection,
    vertical_modes,
    mode_rates,
):
    slots, cycles, _, parts, fields, levels_local = grid.shape
    columns = parts * fields * levels_local
    k_half = legendre.shape[3]
    widths = (k_half + LANE_PAD, k_half)
    held = jnp.transpose(grid, (1, 2, 3, 4, 5, 0)).reshape(cycles, 2, columns, slots)
    hbm = pl.BlockSpec(memory_space=pltpu.HBM)
    packs = [pltpu.VMEM((n_lev, GROUP, width), BF16) for width in widths]
    out = pl.pallas_call(
        functools.partial(step_kernel, n_lat, n_lev),
        out_shape=jax.ShapeDtypeStruct((cycles, 2, columns, slots), BF16),
        in_specs=[hbm] * 9,
        out_specs=hbm,
        scratch_shapes=[
            pltpu.VMEM(held.shape, BF16),
            pltpu.VMEM(legendre.shape, BF16),
            pltpu.SMEM(quad_weights.shape, F32),
            pltpu.SMEM(cycle_points.shape, jnp.int32),
            pltpu.SMEM(wave_ids.shape, jnp.int32),
            pltpu.VMEM((1, slots), jnp.int32),
            pltpu.VMEM(mode_projection.shape, BF16),
            pltpu.VMEM(vertical_modes.shape, BF16),
            pltpu.VMEM((1, mode_rates.shape[0]), F32),
            pltpu.VMEM((2, cycles, slots, columns), F32),
            pltpu.VMEM((cycles, columns, slots), F32),
            pltpu.VMEM((2, slots, cycles, columns), BF16),
            pltpu.VMEM((2, 2, n_lat * cycles, columns), BF16),
            *packs,
            *packs,
            *packs,
            *packs,
            pltpu.VMEM((2, 2, n_lat * cycles, columns), BF16),
            pltpu.VMEM((2, slots, cycles, columns), BF16),
            *[pltpu.VMEM((k_half, width), BF16) for width in widths],
            pltpu.SemaphoreType.DMA((cycles,)),
            pltpu.SemaphoreType.DMA((8,)),
            pltpu.SemaphoreType.DMA((4, 2)),
            pltpu.SemaphoreType.DMA((4, 2)),
        ],
        compiler_params=pltpu.CompilerParams(
            collective_id=0, has_side_effects=True, vmem_limit_bytes=62914560
        ),
        name="spectral_step",
    )(
        held,
        legendre,
        quad_weights,
        cycle_points,
        wave_ids,
        wave_ids.reshape(1, slots),
        mode_projection,
        vertical_modes,
        mode_rates.reshape(1, -1),
    )
    out = out.reshape(cycles, 2, parts, fields, levels_local, slots)
    return jnp.transpose(out, (5, 0, 1, 2, 3, 4))


def solution(mesh):
    placed = (
        P(None, "lat", None, None, None, "lev"),
        P("lat", None, None, None),
        P("lat"),
        P("lat"),
        P(),
        P(),
        P(),
        P(),
    )
    return jax.shard_map(
        functools.partial(local, mesh.shape["lat"], mesh.shape["lev"]),
        mesh=mesh,
        in_specs=placed,
        out_specs=P(None, "lat", None, None, None, "lev"),
        check_vma=False,
    )
```

```python
import functools

import jax
import jax.numpy as jnp
from jax import lax
from jax.experimental import pallas as pl
from jax.experimental.pallas import tpu as pltpu
from jax.sharding import PartitionSpec as P

MESH = pl.DeviceIdType.MESH
coupling = 2.0
GROUP = 8
LANE_PAD = 128
F32 = jnp.float32
BF16 = jnp.bfloat16


def matmul(a, b):
    return lax.dot_general(a, b, (((1,), (0,)), ((), ())), preferred_element_type=F32)


def matmul_nt(a, b):
    return lax.dot_general(a, b, (((1,), (1,)), ((), ())), preferred_element_type=F32)


def iotas(shape):
    return lax.broadcasted_iota(jnp.int32, shape, 0), lax.broadcasted_iota(jnp.int32, shape, 1)


def unit(condition):
    return jnp.where(condition, 1.0, 0.0).astype(BF16)


def step_kernel(
    n_lat,
    n_lev,
    grid_hbm,
    leg_hbm,
    quad_hbm,
    cycle_hbm,
    wave_hbm,
    wave_row_hbm,
    project_hbm,
    modes_hbm,
    rate_hbm,
    out_hbm,
    grid_ref,
    leg,
    quad_ref,
    cycle_ref,
    wave_ref,
    wave_row_ref,
    project_ref,
    modes_ref,
    rate_ref,
    turned,
    even_ref,
    send,
    recv,
    pack_send_0,
    pack_send_1,
    pack_recv_0,
    pack_recv_1,
    solve_send_0,
    solve_send_1,
    solve_recv_0,
    solve_recv_1,
    back_send,
    back_recv,
    flip_0,
    flip_1,
    grid_sem,
    input_sem,
    send_sem,
    recv_sem,
):
    lat, lev = lax.axis_index("lat"), lax.axis_index("lev")
    cycles, _, columns, slots = grid_hbm.shape
    k_half = leg.shape[3]
    mode_total = 2 * k_half
    rows = cycles * GROUP
    groups = slots // GROUP
    levels = project_ref.shape[0]
    pack_send = (pack_send_0, pack_send_1)
    pack_recv = (pack_recv_0, pack_recv_1)
    solve_send = (solve_send_0, solve_send_1)
    solve_recv = (solve_recv_0, solve_recv_1)
    flips = (flip_0, flip_1)

    def grid_copy(j):
        return pltpu.make_async_copy(grid_hbm.at[j], grid_ref.at[j], grid_sem.at[j])

    inputs = [
        (wave_row_hbm, wave_row_ref),
        (cycle_hbm, cycle_ref),
        (quad_hbm, quad_ref),
        (wave_hbm, wave_ref),
        (leg_hbm, leg),
        (project_hbm, project_ref),
        (modes_hbm, modes_ref),
        (rate_hbm, rate_ref),
    ]
    copies = [
        pltpu.make_async_copy(source, target, input_sem.at[i])
        for i, (source, target) in enumerate(inputs)
    ]
    for copy in copies[:3]:
        copy.start()

    @pl.loop(0, cycles)
    def _(j):
        grid_copy(j).start()

    for copy in copies[3:]:
        copy.start()

    barrier = pltpu.get_barrier_semaphore()

    @pl.loop(1, n_lat)
    def _(r):
        pl.semaphore_signal(
            barrier, inc=1, device_id=(lax.rem(lat + r, n_lat), lev), device_id_type=MESH
        )

    @pl.loop(1, n_lev)
    def _(r):
        pl.semaphore_signal(
            barrier, inc=1, device_id=(lat, lax.rem(lev + r, n_lev)), device_id_type=MESH
        )


    row, col = iotas((columns, columns))
    eye_columns = unit(row == col)
    row, col = iotas((slots, slots))
    eye_slots = unit(row == col)
    row, col = iotas((rows, rows))
    spread = unit(col == (row % cycles) * GROUP + row // cycles)
    collect = unit(col == (row % GROUP) * cycles + row // GROUP)

    x_size = min(8, n_lat // 2)
    y_size = n_lat // (2 * x_size)
    at_core, at_x, at_y = lax.rem(lat, 2), lax.rem(lat // 2, x_size), lat // (2 * x_size)
    near_last = sorted(range(x_size), key=lambda d: -min(d, x_size - d))
    if x_size == 8:
        split_forward = ((3, 5, 2, 6, 1), (4, 7, 0))
        split_return = ((3, 5), (4, 2, 6, 1, 7, 0))
    else:
        split_forward = split_return = (near_last[:-1], near_last[-1:])

    def exchange_lat(stage, p, shifts, source, target):
        for shift in shifts:
            to_x = lax.rem(at_x + shift, x_size)

            @pl.loop(0 if shift else 1, 2 * y_size)
            def _(t):
                to_y = lax.rem(at_y + t // 2, y_size)
                peer = (to_y * x_size + to_x) * 2 + lax.rem(at_core + t, 2)
                pltpu.make_async_remote_copy(
                    src_ref=source(peer),
                    dst_ref=target(lat),
                    send_sem=send_sem.at[stage, p],
                    recv_sem=recv_sem.at[stage, p],
                    device_id=(peer, lev),
                    device_id_type=MESH,
                ).start()

    z_size = n_lev // 2
    at_z, at_half = lax.rem(lev, z_size), lev // z_size
    hops = sorted(range(z_size), key=lambda d: -min(d, z_size - d))
    lev_steps = [(half, hop) for half in (1, 0) for hop in hops if half or hop]

    def exchange_lev(stage, p, source, target):
        for half, hop in lev_steps:
            peer = lax.rem(at_half + half, 2) * z_size + lax.rem(at_z + hop, z_size)
            pltpu.make_async_remote_copy(
                src_ref=source.at[peer],
                dst_ref=target.at[lev],
                send_sem=send_sem.at[stage, p],
                recv_sem=recv_sem.at[stage, p],
                device_id=(lat, peer),
                device_id_type=MESH,
            ).start()

    def wait_all(view, semaphore):
        pltpu.make_async_copy(view, view, semaphore).wait()

    def lat_view(p):
        return send.at[p, pl.ds(0, slots - 2)]

    def lev_view(p):
        return pack_send[p].at[pl.ds(0, n_lev - 1)]

    def own_rows(index):
        return pl.ds(pl.multiple_of(index * cycles, cycles), cycles)

    def fold(p):
        @pl.loop(0, cycles, unroll=4)
        def _(j):
            if p == 0:
                grid_copy(j).wait()
            present = jnp.where(2 * wave_row_ref[...] < cycle_ref[j], quad_ref[j], 0.0)
            north = grid_ref[j, 0].astype(F32)
            south = grid_ref[j, 1].astype(F32)
            total = north + south if p == 0 else north - south
            turned[p, j] = matmul_nt(eye_slots, (present * total).astype(BF16))

        @pl.loop(0, groups, unroll=4)
        def _(g):
            block = turned[p, :, pl.ds(pl.multiple_of(g * GROUP, GROUP), GROUP), :]
            block = block.reshape(rows, columns).astype(BF16)
            moved = matmul(spread, block).astype(BF16)
            send[p, pl.ds(g * GROUP, GROUP)] = moved.reshape(GROUP, cycles, columns)

    def send_fold(p, shifts):
        exchange_lat(
            0,
            p,
            shifts,
            lambda peer: send.at[p, pl.ds(2 * peer, 2)],
            lambda me: recv.at[p, :, own_rows(me), :],
        )

    def keep_fold(p):
        for slot in range(2):
            recv[p, slot, own_rows(lat), :] = send[p, 2 * lat + slot]

    def order(p, slot):
        k_index = lax.broadcasted_iota(jnp.int32, (1, k_half), 1)
        return wave_ref[2 * lat + slot] + p + 2 * k_index

    def forward(p):
        wait_all(lat_view(p), recv_sem.at[0, p])
        parts = []
        for slot in range(2):
            across = matmul_nt(eye_columns, recv[p, slot]).astype(BF16)
            spectral = matmul(across, leg[slot, p])
            parts.append(jnp.where(order(p, slot) <= mode_total - 1, spectral, 0.0))
        flipped = matmul(parts[1].astype(BF16), flips[p][...])
        packed = flipped[:, :k_half] + parts[0]
        pack_send[p][:, :, :k_half] = packed.reshape(n_lev, GROUP, k_half).astype(BF16)
        if flipped.shape[1] > k_half:
            rest = flipped[:, k_half:]
            pack_send[p][:, :, k_half:] = rest.reshape(n_lev, GROUP, -1).astype(BF16)
        exchange_lev(1, p, pack_send[p], pack_recv[p])
        pack_recv[p][lev] = pack_send[p][lev]

    def solve(p):
        wait_all(lev_view(p), recv_sem.at[1, p])
        packed = pack_recv[p][...].astype(F32).reshape(levels, -1).astype(BF16)
        width = packed.shape[1]
        q_index = lax.broadcasted_iota(jnp.int32, (1, width), 1)
        first = wave_ref[2 * lat] + p + 2 * q_index
        second = wave_ref[2 * lat + 1] + p + 2 * (k_half - p - q_index)
        total_order = jnp.where(first <= mode_total - 1, first, second).astype(F32)
        growth = coupling * total_order * (total_order + 1.0) / (mode_total * mode_total)
        rates = jnp.transpose(jnp.broadcast_to(rate_ref[...], (levels, levels)))[:, :1]
        projected = matmul(project_ref[...], packed)
        damped = (projected / (1.0 + growth * rates)).astype(BF16)
        solved = matmul(modes_ref[...], damped)
        solve_send[p][...] = solved.reshape(n_lev, GROUP, width).astype(BF16)
        exchange_lev(2, p, solve_send[p], solve_recv[p])
        solve_recv[p][lev] = solve_send[p][lev]

    def inverse(p):
        wait_all(lev_view(p), recv_sem.at[2, p])
        packed = solve_recv[p][...].astype(F32).reshape(columns, -1)
        unpacked = (packed[:, :k_half], matmul_nt(packed.astype(BF16), flips[p][...]))
        for slot in range(2):
            coeffs = jnp.where(order(p, slot) <= mode_total - 1, unpacked[slot], 0.0)
            back_send[p, slot] = matmul_nt(leg[slot, p], coeffs.astype(BF16)).astype(BF16)

    def send_back(p, shifts):
        exchange_lat(
            3,
            p,
            shifts,
            lambda peer: back_send.at[p, :, own_rows(peer), :],
            lambda me: back_recv.at[p, pl.ds(2 * me, 2)],
        )

    def keep_back(p):
        for slot in range(2):
            back_recv[p, 2 * lat + slot] = back_send[p, slot, own_rows(lat), :]

    def spread_back(p):
        wait_all(lat_view(p), recv_sem.at[3, p])

        @pl.loop(0, groups, unroll=4)
        def _(g):
            block = back_recv[p, pl.ds(g * GROUP, GROUP)].reshape(rows, columns)
            moved = matmul(collect, block).reshape(cycles, GROUP, columns)
            turned[p, :, pl.ds(pl.multiple_of(g * GROUP, GROUP), GROUP), :] = moved

    def cross(p, j):
        return matmul_nt(eye_columns, turned[p, j].astype(BF16))

    def out_copy(j):
        return pltpu.make_async_copy(grid_ref.at[j], out_hbm.at[j], grid_sem.at[j])

    def turn_even():
        @pl.loop(0, cycles, unroll=4)
        def _(j):
            even_ref[j] = cross(0, j)

    def unfold():
        @pl.loop(0, cycles, unroll=4)
        def _(j):
            present = jnp.where(2 * wave_row_ref[...] < cycle_ref[j], 1.0, 0.0)
            even, odd = even_ref[j], cross(1, j)
            grid_ref[j, 0] = (present * (even + odd)).astype(BF16)
            grid_ref[j, 1] = (present * (even - odd)).astype(BF16)
            out_copy(j).start()

    for copy in copies[:3]:
        copy.wait()
    fold(0)
    pl.semaphore_wait(barrier, n_lat + n_lev - 2)
    send_fold(0, near_last)
    keep_fold(0)
    fold(1)
    send_fold(1, split_forward[0])
    keep_fold(1)
    for p in range(2):
        row, col = iotas(flips[p].shape)
        flips[p][...] = unit(row + col == k_half - p)
    for copy in copies[3:]:
        copy.wait()
    forward(0)
    send_fold(1, split_forward[1])
    solve(0)
    forward(1)
    inverse(0)
    send_back(0, split_return[0])
    keep_back(0)
    solve(1)
    send_back(0, split_return[1])
    inverse(1)
    send_back(1, near_last)
    keep_back(1)
    spread_back(0)
    turn_even()
    spread_back(1)
    unfold()
    for p in range(2):
        wait_all(lat_view(p), send_sem.at[0, p])
        wait_all(lev_view(p), send_sem.at[1, p])
        wait_all(lev_view(p), send_sem.at[2, p])
        wait_all(lat_view(p), send_sem.at[3, p])

    @pl.loop(0, cycles)
    def _(j):
        out_copy(j).wait()


def local(
    n_lat,
    n_lev,
    grid,
    legendre,
    quad_weights,
    cycle_points,
    wave_ids,
    mode_projection,
    vertical_modes,
    mode_rates,
):
    slots, cycles, _, parts, fields, levels_local = grid.shape
    columns = parts * fields * levels_local
    k_half = legendre.shape[3]
    widths = (k_half + LANE_PAD, k_half)
    held = jnp.transpose(grid, (1, 2, 3, 4, 5, 0)).reshape(cycles, 2, columns, slots)
    hbm = pl.BlockSpec(memory_space=pltpu.HBM)
    packs = [pltpu.VMEM((n_lev, GROUP, width), BF16) for width in widths]
    out = pl.pallas_call(
        functools.partial(step_kernel, n_lat, n_lev),
        out_shape=jax.ShapeDtypeStruct((cycles, 2, columns, slots), BF16),
        in_specs=[hbm] * 9,
        out_specs=hbm,
        scratch_shapes=[
            pltpu.VMEM(held.shape, BF16),
            pltpu.VMEM(legendre.shape, BF16),
            pltpu.SMEM(quad_weights.shape, F32),
            pltpu.SMEM(cycle_points.shape, jnp.int32),
            pltpu.SMEM(wave_ids.shape, jnp.int32),
            pltpu.VMEM((1, slots), jnp.int32),
            pltpu.VMEM(mode_projection.shape, BF16),
            pltpu.VMEM(vertical_modes.shape, BF16),
            pltpu.VMEM((1, mode_rates.shape[0]), F32),
            pltpu.VMEM((2, cycles, slots, columns), F32),
            pltpu.VMEM((cycles, columns, slots), F32),
            pltpu.VMEM((2, slots, cycles, columns), BF16),
            pltpu.VMEM((2, 2, n_lat * cycles, columns), BF16),
            *packs,
            *packs,
            *packs,
            *packs,
            pltpu.VMEM((2, 2, n_lat * cycles, columns), BF16),
            pltpu.VMEM((2, slots, cycles, columns), BF16),
            *[pltpu.VMEM((k_half, width), BF16) for width in widths],
            pltpu.SemaphoreType.DMA((cycles,)),
            pltpu.SemaphoreType.DMA((8,)),
            pltpu.SemaphoreType.DMA((4, 2)),
            pltpu.SemaphoreType.DMA((4, 2)),
        ],
        compiler_params=pltpu.CompilerParams(
            collective_id=0, has_side_effects=True, vmem_limit_bytes=62914560
        ),
        name="spectral_step",
    )(
        held,
        legendre,
        quad_weights,
        cycle_points,
        wave_ids,
        wave_ids.reshape(1, slots),
        mode_projection,
        vertical_modes,
        mode_rates.reshape(1, -1),
    )
    out = out.reshape(cycles, 2, parts, fields, levels_local, slots)
    return jnp.transpose(out, (5, 0, 1, 2, 3, 4))


def solution(mesh):
    placed = (
        P(None, "lat", None, None, None, "lev"),
        P("lat", None, None, None),
        P("lat"),
        P("lat"),
        P(),
        P(),
        P(),
        P(),
    )
    return jax.shard_map(
        functools.partial(local, mesh.shape["lat"], mesh.shape["lev"]),
        mesh=mesh,
        in_specs=placed,
        out_specs=P(None, "lat", None, None, None, "lev"),
        check_vma=False,
    )
```
